32 devices in a mesh: gy: 4 (over y, x), gx: 8 (over z, core).
Axes of the slice: x: 2, y: 2, z: 4, core: 2. Of those that a mesh axis runs over, the one named last changes fastest.
Arguments:
- u_field: float32 [8, 512, 1024], P(None, 'gx', 'gy')
- v_field: float32 [8, 512, 1024], P(None, 'gx', 'gy')
- w_field: float32 [8, 512, 1024], P(None, 'gx', 'gy')
- sep_x: int32 [16], replicated, may hold values from 1 to 128, as said below
- sep_y: int32 [16], replicated, may hold values from 1 to 256, as said below
- sep_z: int32 [16], replicated, may hold values from 1 to 4
Outputs:
- correlation: float32 [3, 16], replicated
The draws below stay inside these ranges and needn't reach their ends.
Inputs may be any that keep to these rules, and one draw needn't show every extreme that they name: `sep_x`: every separation along x lies in 1 to 128, and 128 is among them in every draw; repeats may occur. `sep_y`: every separation along y lies in 1 to 256, and 256 is among them in every draw; repeats may occur.
All inputs are finite; a program needn't handle non-finite values.
Results may differ from the reference program's by a relative error of at most 0.0003.
Values sent between devices are 32-bit elements; how exact they have to be, the bound alone decides.
A program may use at most 64 MiB of HBM per device.

```python
import math
import jax
import jax.numpy as jnp
from jax import lax

PLANES = 8
CX = 64
CY = 256
SEPS = 16
NX = 512
NY = 1024


def rough_scale(key, shape, spread):
    return jnp.exp(jax.random.uniform(key, shape, jnp.float32, -spread, spread))


def smooth_field(key, salt_value):
    key = jax.random.fold_in(key, salt_value)
    key_list = jax.random.split(key, 12)
    mode_count = 6
    plane_pos = jnp.arange(PLANES, dtype=jnp.float32)[:, None, None]
    row_pos = jnp.arange(NX, dtype=jnp.float32)[None, :, None]
    column_pos = jnp.arange(NY, dtype=jnp.float32)[None, None, :]
    wave_x = jax.random.randint(key_list[0], (mode_count,), 1, 5).astype(jnp.float32)
    wave_y = jax.random.randint(key_list[1], (mode_count,), 1, 5).astype(jnp.float32)
    wave_z = jax.random.randint(key_list[2], (mode_count,), 0, 3).astype(jnp.float32)
    phases = jax.random.uniform(key_list[3], (mode_count, 3), jnp.float32, 0.0, 2.0 * math.pi)
    amplitude = jax.random.uniform(key_list[4], (mode_count,), jnp.float32, 0.5, 1.0)
    smooth = jnp.zeros((PLANES, NX, NY), jnp.float32)
    for mode_index in range(mode_count):
        cos_x = jnp.cos(2.0 * math.pi * wave_x[mode_index] * row_pos / NX + phases[mode_index, 0])
        cos_y = jnp.cos(2.0 * math.pi * wave_y[mode_index] * column_pos / NY + phases[mode_index, 1])
        cos_z = jnp.cos(2.0 * math.pi * wave_z[mode_index] * plane_pos / (4.0 * PLANES) + phases[mode_index, 2])
        smooth = smooth + amplitude[mode_index] * cos_x * cos_y * cos_z
    spread = 1.15
    noise_part = 0.7 * jax.random.normal(key_list[11], (PLANES, NX, NY), jnp.float32)
    smooth_scale = rough_scale(key_list[5], (PLANES, 1, 1), spread) * rough_scale(key_list[6], (1, NX, 1), spread) * rough_scale(key_list[7], (1, 1, NY), spread)
    noise_scale = rough_scale(key_list[8], (PLANES, 1, 1), spread) * rough_scale(key_list[9], (1, NX, 1), spread) * rough_scale(key_list[10], (1, 1, NY), spread)
    return smooth_scale * (1.5 * smooth) + noise_scale * noise_part


def draw_u_field(key, part):
    return smooth_field(key, 11)


def draw_v_field(key, part):
    return smooth_field(key, 23)


def draw_w_field(key, part):
    return smooth_field(key, 37)


def separations(key, salt_value, largest):
    key = jax.random.fold_in(key, salt_value)
    key_list = jax.random.split(key, 2)
    others = jax.random.randint(key_list[0], (SEPS - 1,), 1, largest + 1)
    values = jnp.concatenate([others, jnp.full((1,), largest, jnp.int32)])
    return jax.random.permutation(key_list[1], values).astype(jnp.int32)


def draw_sep_x(key, part):
    return separations(key, 41, 2 * CX)


def draw_sep_y(key, part):
    return separations(key, 53, CY)


def touch_ends(drawn, stream_key, smallest, top_value):
    dims = drawn.shape
    index_at = [jax.random.randint(jax.random.fold_in(stream_key, axis), (), 0, dims[axis]) for axis in range(len(dims))]
    drawn = drawn.at[tuple(index_at)].set(smallest)
    longest = dims.index(max(dims))
    index_at[longest] = (index_at[longest] + 1) % dims[longest]
    return drawn.at[tuple(index_at)].set(top_value)


def setup_inputs(seed: int = 0) -> dict:
    streams_of = jax.random.split(jax.random.key(seed), 7)
    u_field = draw_u_field(jax.random.fold_in(streams_of[6], 71), 0)
    v_field = draw_v_field(jax.random.fold_in(streams_of[6], 71), 0)
    w_field = draw_w_field(jax.random.fold_in(streams_of[6], 71), 0)
    sep_x = draw_sep_x(jax.random.fold_in(streams_of[6], 71), 0)
    sep_y = draw_sep_y(jax.random.fold_in(streams_of[6], 71), 0)
    sep_z = touch_ends(jax.random.randint(streams_of[5], (SEPS,), 1, PLANES // 2 + 1), jax.random.fold_in(streams_of[5], 1), 1, (PLANES // 2 + 1) - 1).astype(jnp.int32)
    return {"u_field": u_field, "v_field": v_field, "w_field": w_field, "sep_x": sep_x, "sep_y": sep_y, "sep_z": sep_z}


def reference(u_field, v_field, w_field, sep_x, sep_y, sep_z):
    planes = u_field.shape[0]

    def along_x(lag_value):
        return jnp.sum(u_field * jnp.roll(u_field, -lag_value, axis=1))

    def along_y(lag_value):
        return jnp.sum(v_field * jnp.roll(v_field, -lag_value, axis=2))

    padded = jnp.concatenate([w_field, jnp.zeros_like(w_field)], axis=0)

    def along_z(lag_value):
        shifted = lax.dynamic_slice_in_dim(padded, lag_value.astype(jnp.int32), planes, 0)
        return jnp.sum(w_field * shifted)

    sums_x = lax.map(along_x, sep_x)
    sums_y = lax.map(along_y, sep_y)
    sums_z = lax.map(along_z, sep_z)
    energy_u = jnp.sum(u_field * u_field)
    energy_v = jnp.sum(v_field * v_field)
    energy_w = jnp.sum(w_field * w_field)
    factor = jnp.float32(planes) / (jnp.float32(planes) - sep_z.astype(jnp.float32))
    row_x = sums_x / energy_u
    row_y = sums_y / energy_v
    row_z = sums_z / energy_w * factor
    return jnp.stack([row_x, row_y, row_z], axis=0)
```

```python
import functools

import jax
import jax.numpy as jnp
from jax import lax
from jax.experimental import pallas as pl
from jax.experimental.pallas import tpu as pltpu
from jax.sharding import PartitionSpec as P

MESH = pl.DeviceIdType.MESH
LANES = 128
FIELD_LANES = 32


def split(value):
    high = value.astype(jnp.bfloat16)
    low = (value - high.astype(jnp.float32)).astype(jnp.bfloat16)
    return high, low


def product(left, right, dims):
    dot = functools.partial(
        lax.dot_general, dimension_numbers=(dims, ((), ())), preferred_element_type=jnp.float32
    )
    return dot(left[0], right[0]) + (dot(left[0], right[1]) + dot(left[1], right[0]))


def diagonal_sums(gram, largest):
    rows = gram.shape[0]
    window = largest + LANES
    folded = gram[:LANES, :window]
    for start in range(LANES, rows, LANES):
        folded = folded + gram[start : start + LANES, start : start + window]
    total = folded[:8]
    for start in range(8, LANES, 8):
        total = total + pltpu.roll(folded[start : start + 8], window - start, 1)
    row = lax.broadcasted_iota(jnp.int32, total.shape, 0)
    for bit in (1, 2, 4):
        total = jnp.where((row & bit) != 0, pltpu.roll(total, window - bit, 1), total)
    return total


def kernel(
    n_gx, n_gy,
    u_hbm, v_hbm, w_hbm, sep_x_hbm, sep_y_hbm, sep_z_hbm, out_ref,
    u_own, v_own, w_own, u_wide, v_wide, sep_s, gx_rows, gy_rows,
    load_sem, sep_sem, place_sem, u_send, u_recv, d_send, d_recv, v_send, v_recv,
    gx_send, gx_recv, gy_send, gy_recv,
):
    planes, width_x, width_y = u_own.shape
    seps = sep_s.shape[1]
    quarter, half = planes // 4, planes // 2
    gx, gy = lax.axis_index("gx"), lax.axis_index("gy")
    core, parity = lax.rem(gx, 2), lax.rem(gy, 2)
    chip_first = gx - core

    load_u = pltpu.make_async_copy(u_hbm, u_own, load_sem.at[0])
    load_v = pltpu.make_async_copy(v_hbm, v_own, load_sem.at[1])
    load_w = pltpu.make_async_copy(w_hbm, w_own, load_sem.at[2])
    load_u.start()
    load_v.start()

    barrier = pltpu.get_barrier_semaphore()
    for step in range(1, n_gx):
        pl.semaphore_signal(
            barrier, inc=1, device_id={"gx": lax.rem(gx + step, n_gx)}, device_id_type=MESH
        )
    for step in range(1, n_gy):
        pl.semaphore_signal(
            barrier, inc=1, device_id={"gy": lax.rem(gy + step, n_gy)}, device_id_type=MESH
        )
    load_w.start()
    sep_loads = [
        pltpu.make_async_copy(ref, sep_s.at[index], sep_sem.at[index])
        for index, ref in enumerate((sep_x_hbm, sep_y_hbm, sep_z_hbm))
    ]
    places = []
    for side in range(2):
        places.append(pltpu.make_async_copy(
            u_hbm.at[pl.ds(half * side + quarter * core, quarter)],
            u_wide.at[side, :, 2 * side + core],
            place_sem.at[side],
        ))
    places.append(pltpu.make_async_copy(
        v_hbm.at[pl.ds(half * parity, half)], v_wide.at[2 * parity], place_sem.at[2]
    ))
    for copy in places + sep_loads:
        copy.start()

    u_copies = []
    for item in range(quarter):
        for other in range(2):
            for side in range(2):
                chip = lax.rem(chip_first + (n_gx - 2 if side == 0 else 2), n_gx)
                u_copies.append(pltpu.make_async_remote_copy(
                    src_ref=u_own.at[half * side + quarter * other + item],
                    dst_ref=u_wide.at[side, item, (2 if side == 0 else 0) + core],
                    send_sem=u_send.at[side, item, other],
                    recv_sem=u_recv.at[side, item, core],
                    device_id={"gx": chip + other},
                    device_id_type=MESH,
                ))
    d_copies = []
    for side in range(2):
        d_copies.append(pltpu.make_async_remote_copy(
            src_ref=u_own.at[pl.ds(half * side + quarter * (1 - core), quarter)],
            dst_ref=u_wide.at[side, :, 2 * side + core],
            send_sem=d_send.at[side],
            recv_sem=d_recv.at[side],
            device_id={"gx": chip_first + 1 - core},
            device_id_type=MESH,
        ))
    near = gy + 1 - 2 * parity
    far = lax.rem(gy + n_gy - 2 + 4 * parity, n_gy)
    v_copies = []
    for item in range(half):
        v_copies.append(pltpu.make_async_remote_copy(
            src_ref=v_own.at[half * (1 - parity) + item],
            dst_ref=v_wide.at[1, item],
            send_sem=v_send.at[0, item],
            recv_sem=v_recv.at[0, item],
            device_id={"gy": near},
            device_id_type=MESH,
        ))
        v_copies.append(pltpu.make_async_remote_copy(
            src_ref=v_own.at[half * parity + item],
            dst_ref=v_wide.at[2 - 2 * parity, item],
            send_sem=v_send.at[1, item],
            recv_sem=v_recv.at[1, item],
            device_id={"gy": far},
            device_id_type=MESH,
        ))

    load_u.wait()
    load_v.wait()
    pl.semaphore_wait(barrier, n_gx + n_gy - 2)
    for copy in u_copies + v_copies + d_copies:
        copy.start()

    for copy in sep_loads:
        copy.wait()
    lane = lax.broadcasted_iota(jnp.int32, (1, LANES), 1)
    lag_row = jnp.full((1, LANES), -1, jnp.int32)
    for field in range(3):
        for index in range(seps):
            lag_row = jnp.where(lane == FIELD_LANES * field + index, sep_s[field, index], lag_row)
        lag_row = jnp.where(lane == FIELD_LANES * field + seps, 0, lag_row)

    def picker(field, lags):
        of_field = (lane >= FIELD_LANES * field) & (lane < FIELD_LANES * (field + 1))
        wanted = jnp.where(of_field, lag_row, -1)
        lag = lax.broadcasted_iota(jnp.int32, (lags, LANES), 0)
        return jnp.where(lag == wanted, 1.0, 0.0).astype(jnp.float32)

    def pick(sums, field):
        return jnp.dot(
            sums, picker(field, sums.shape[1]),
            precision=lax.Precision.HIGHEST, preferred_element_type=jnp.float32,
        )

    load_w.wait()
    lags_z = half + 1
    tile_rows = 8

    def z_step(index, carry):
        start = pl.multiple_of(index * tile_rows, tile_rows)
        rows = [w_own[plane, pl.ds(start, tile_rows), :] for plane in range(planes)]
        return tuple(
            carry[lag] + sum(rows[plane] * rows[plane + lag] for plane in range(planes - lag))
            for lag in range(lags_z)
        )

    zero = jnp.zeros((tile_rows, width_y), jnp.float32)
    z_sums = lax.fori_loop(0, width_x // tile_rows, z_step, (zero,) * lags_z)
    row_z = jnp.zeros((1, LANES), jnp.float32)
    for lag in range(lags_z):
        row_z = jnp.where(lag_row == lag, jnp.sum(z_sums[lag]), row_z)
    row_z = jnp.where((lane >= 2 * FIELD_LANES) & (lane < 3 * FIELD_LANES), row_z, 0.0)

    for copy in places:
        copy.wait()
    for copy in v_copies:
        copy.wait_recv()
    cells = half * width_x
    wide = v_wide[...].reshape(3 * cells, width_y)
    high, low = split(wide)
    left = (high[: 2 * cells], low[: 2 * cells])
    gram_0 = product(left, left, ((0,), (0,)))
    gram_1 = product(left, (high[cells:], low[cells:]), ((0,), (0,)))
    gram_y = jnp.concatenate([gram_0, gram_1], axis=1)
    part = pick(diagonal_sums(gram_y, width_y), 1)

    for copy in d_copies:
        copy.wait_recv()
    gram_x = None
    for item in range(quarter):
        for side in range(2):
            for sender in range(2):
                slot = (2 if side == 0 else 0) + sender
                pltpu.make_async_remote_copy(
                    src_ref=u_own.at[0],
                    dst_ref=u_wide.at[side, item, slot],
                    send_sem=u_send.at[side, item, sender],
                    recv_sem=u_recv.at[side, item, sender],
                    device_id={"gx": chip_first + 1 - core},
                    device_id_type=MESH,
                ).wait_recv()
            pair = split(u_wide[side, item].reshape(4 * width_x, width_y))
            lower = (pair[0][: 2 * width_x], pair[1][: 2 * width_x])
            term = product(lower, pair, ((1,), (1,)))
            gram_x = term if gram_x is None else gram_x + term
    part = part + pick(diagonal_sums(gram_x, 2 * width_x), 0)
    mine = jnp.sum(part, axis=0, keepdims=True) + row_z

    def all_sum(value, rows_ref, send_sem, recv_sem, axis, me, count):
        rows_ref[me] = value
        copies = []
        for step in range(1, count):
            copies.append(pltpu.make_async_remote_copy(
                src_ref=rows_ref.at[me],
                dst_ref=rows_ref.at[me],
                send_sem=send_sem.at[step],
                recv_sem=recv_sem.at[step],
                device_id={axis: lax.rem(me + step, count)},
                device_id_type=MESH,
            ))
        for copy in copies:
            copy.start()
        for copy in copies:
            copy.wait_recv()
        total = rows_ref[0]
        for index in range(1, count):
            total = total + rows_ref[index]
        return total, copies

    total, copies_gx = all_sum(mine, gx_rows, gx_send, gx_recv, "gx", gx, n_gx)
    total, copies_gy = all_sum(total, gy_rows, gy_send, gy_recv, "gy", gy, n_gy)

    for field in range(3):
        base = FIELD_LANES * field
        row = total[:, base : base + seps] / total[:, base + seps : base + seps + 1]
        if field == 2:
            lag = lag_row[:, base : base + seps].astype(jnp.float32)
            row = row * (jnp.float32(planes) / (jnp.float32(planes) - lag))
        out_ref[field : field + 1, :] = row

    for copy in u_copies + v_copies + d_copies + copies_gx + copies_gy:
        copy.wait_send()


def local(n_gx, n_gy, u_field, v_field, w_field, sep_x, sep_y, sep_z):
    planes, width_x, width_y = u_field.shape
    quarter, half = planes // 4, planes // 2
    seps = sep_x.shape[0]
    dma = pltpu.SemaphoreType.DMA
    block = (planes, width_x, width_y)
    return pl.pallas_call(
        functools.partial(kernel, n_gx, n_gy),
        out_shape=jax.ShapeDtypeStruct((3, seps), jnp.float32),
        in_specs=[pl.BlockSpec(memory_space=pl.ANY)] * 6,
        out_specs=pl.BlockSpec(memory_space=pltpu.VMEM),
        scratch_shapes=[
            pltpu.VMEM(block, jnp.float32),
            pltpu.VMEM(block, jnp.float32),
            pltpu.VMEM(block, jnp.float32),
            pltpu.VMEM((2, quarter, 4, width_x, width_y), jnp.float32),
            pltpu.VMEM((3, half, width_x, width_y), jnp.float32),
            pltpu.SMEM((3, seps), jnp.int32),
            pltpu.VMEM((n_gx, 1, LANES), jnp.float32),
            pltpu.VMEM((n_gy, 1, LANES), jnp.float32),
            dma((3,)),
            dma((3,)),
            dma((3,)),
            dma((2, quarter, 2)),
            dma((2, quarter, 2)),
            dma((2,)),
            dma((2,)),
            dma((2, half)),
            dma((2, half)),
            dma((n_gx,)),
            dma((n_gx,)),
            dma((n_gy,)),
            dma((n_gy,)),
        ],
        compiler_params=pltpu.CompilerParams(collective_id=0, has_side_effects=True),
    )(u_field, v_field, w_field, sep_x, sep_y, sep_z)


def solution(mesh):
    return jax.shard_map(
        functools.partial(local, mesh.shape["gx"], mesh.shape["gy"]),
        mesh=mesh,
        in_specs=(P(None, "gx", "gy"), P(None, "gx", "gy"), P(None, "gx", "gy"), P(), P(), P()),
        out_specs=P(),
        check_vma=False,
    )
```

```python
import functools

import jax
import jax.numpy as jnp
from jax import lax
from jax.experimental import pallas as pl
from jax.experimental.pallas import tpu as pltpu
from jax.sharding import PartitionSpec as P

MESH = pl.DeviceIdType.MESH
LANES = 128
FIELD_LANES = 32


def split(value):
    high = value.astype(jnp.bfloat16)
    low = (value - high.astype(jnp.float32)).astype(jnp.bfloat16)
    return high, low


def product(left, right, dims):
    dot = functools.partial(
        lax.dot_general, dimension_numbers=(dims, ((), ())), preferred_element_type=jnp.float32
    )
    return dot(left[0], right[0]) + (dot(left[0], right[1]) + dot(left[1], right[0]))


def diagonal_sums(gram, largest):
    rows = gram.shape[0]
    window = largest + LANES
    folded = gram[:LANES, :window]
    for start in range(LANES, rows, LANES):
        folded = folded + gram[start : start + LANES, start : start + window]
    total = folded[:8]
    for start in range(8, LANES, 8):
        total = total + pltpu.roll(folded[start : start + 8], window - start, 1)
    row = lax.broadcasted_iota(jnp.int32, total.shape, 0)
    for bit in (1, 2, 4):
        total = jnp.where((row & bit) != 0, pltpu.roll(total, window - bit, 1), total)
    return total


def kernel(
    n_gx, n_gy,
    u_hbm, v_hbm, w_hbm, sep_x_hbm, sep_y_hbm, sep_z_hbm, out_ref,
    u_own, v_own, w_own, u_wide, v_wide, sep_s, rows,
    load_sem, sep_sem, place_sem, u_send, u_recv, d_send, d_recv, v_send, v_recv,
    row_sem, line_sem, pair_sem,
):
    planes, width_x, width_y = u_own.shape
    seps = sep_s.shape[1]
    quarter, half = planes // 4, planes // 2
    gx, gy = lax.axis_index("gx"), lax.axis_index("gy")
    core, parity = lax.rem(gx, 2), lax.rem(gy, 2)
    chip_first = gx - core

    load_u = pltpu.make_async_copy(u_hbm, u_own, load_sem.at[0])
    load_v = pltpu.make_async_copy(v_hbm, v_own, load_sem.at[1])
    load_w = pltpu.make_async_copy(w_hbm, w_own, load_sem.at[2])
    load_u.start()
    load_v.start()

    chip, chips = gx // 2, n_gx // 2
    first, last = chip == 0, chip == chips - 1
    near = gy + 1 - 2 * parity
    far_to = lax.rem(gy + n_gy - 2 + 4 * parity, n_gy)
    far_from = lax.rem(gy + n_gy + 2 - 4 * parity, n_gy)
    barrier = pltpu.get_barrier_semaphore()

    def greet(semaphore, **device):
        pl.semaphore_signal(semaphore, inc=1, device_id=device, device_id_type=MESH)

    @pl.when(~first)
    def _():
        greet(barrier, gx=chip_first - 2)
        greet(barrier, gx=chip_first - 1)

    @pl.when(~last)
    def _():
        greet(barrier, gx=chip_first + 2)
        greet(barrier, gx=chip_first + 3)

    greet(barrier, gx=chip_first + 1 - core)
    greet(barrier, gy=near)
    greet(barrier, gy=far_from)
    load_w.start()
    sep_loads = [
        pltpu.make_async_copy(ref, sep_s.at[index], sep_sem.at[index])
        for index, ref in enumerate((sep_x_hbm, sep_y_hbm, sep_z_hbm))
    ]
    places = []
    for side in range(2):
        places.append(pltpu.make_async_copy(
            u_hbm.at[pl.ds(half * side + quarter * core, quarter)],
            u_wide.at[side, :, 2 * side + core],
            place_sem.at[side],
        ))
    places.append(pltpu.make_async_copy(
        v_hbm.at[pl.ds(half * parity, half)], v_wide.at[2 * parity], place_sem.at[2]
    ))
    for copy in places + sep_loads:
        copy.start()

    u_copies = {}
    for item in range(quarter):
        for other in range(2):
            for side in range(2):
                target = lax.rem(chip_first + (n_gx - 2 if side == 0 else 2), n_gx)
                u_copies[side, item, other] = (pltpu.make_async_remote_copy(
                    src_ref=u_own.at[half * side + quarter * other + item],
                    dst_ref=u_wide.at[side, item, (2 if side == 0 else 0) + core],
                    send_sem=u_send.at[side, item, other],
                    recv_sem=u_recv.at[side, item, core],
                    device_id={"gx": target + other},
                    device_id_type=MESH,
                ))
    d_copies = []
    for side in range(2):
        d_copies.append(pltpu.make_async_remote_copy(
            src_ref=u_own.at[pl.ds(half * side + quarter * (1 - core), quarter)],
            dst_ref=u_wide.at[side, :, 2 * side + core],
            send_sem=d_send.at[side],
            recv_sem=d_recv.at[side],
            device_id={"gx": chip_first + 1 - core},
            device_id_type=MESH,
        ))
    v_copies = []
    for item in range(half):
        v_copies.append(pltpu.make_async_remote_copy(
            src_ref=v_own.at[half * (1 - parity) + item],
            dst_ref=v_wide.at[1, item],
            send_sem=v_send.at[0, item],
            recv_sem=v_recv.at[0, item],
            device_id={"gy": near},
            device_id_type=MESH,
        ))
        v_copies.append(pltpu.make_async_remote_copy(
            src_ref=v_own.at[half * parity + item],
            dst_ref=v_wide.at[2 - 2 * parity, item],
            send_sem=v_send.at[1, item],
            recv_sem=v_recv.at[1, item],
            device_id={"gy": far_to},
            device_id_type=MESH,
        ))

    load_u.wait()
    load_v.wait()
    inner = jnp.where(first, 0, 2) + jnp.where(last, 0, 2)
    pl.semaphore_wait(barrier, inner + 3)

    def start_u(side, items, at_end):
        wraps = first if side == 0 else last

        @pl.when(wraps if at_end else ~wraps)
        def _():
            for item in items:
                for other in range(2):
                    u_copies[side, item, other].start()

    for side in range(2):
        start_u(side, range(1), False)
    for copy in v_copies + d_copies:
        copy.start()

    up, down = line_sem.at[0], line_sem.at[1]

    @pl.when(chip == 1)
    def _():
        greet(up, gx=gx + 2)

    @pl.when(chip == chips - 2)
    def _():
        greet(down, gx=gx - 2)

    @pl.when(chip >= 2)
    def _():
        pl.semaphore_wait(up, 1)

    @pl.when((chip >= 2) & (chip <= chips - 2))
    def _():
        greet(up, gx=gx + 2)

    @pl.when(chip <= chips - 3)
    def _():
        pl.semaphore_wait(down, 1)

    @pl.when((chip >= 1) & (chip <= chips - 3))
    def _():
        greet(down, gx=gx - 2)

    for side in range(2):
        start_u(side, range(quarter), True)
    for side in range(2):
        start_u(side, range(1, quarter), False)

    greet(pair_sem.at[0], gy=near)
    pl.semaphore_wait(pair_sem.at[0], 1)
    for hop in range(1, n_gy // 2):
        greet(pair_sem.at[hop], gy=far_from)
        pl.semaphore_wait(pair_sem.at[hop], 1)

    for copy in sep_loads:
        copy.wait()
    lane = lax.broadcasted_iota(jnp.int32, (1, LANES), 1)
    lag_row = jnp.full((1, LANES), -1, jnp.int32)
    for field in range(3):
        for index in range(seps):
            lag_row = jnp.where(lane == FIELD_LANES * field + index, sep_s[field, index], lag_row)
        lag_row = jnp.where(lane == FIELD_LANES * field + seps, 0, lag_row)

    def picker(field, lags):
        of_field = (lane >= FIELD_LANES * field) & (lane < FIELD_LANES * (field + 1))
        wanted = jnp.where(of_field, lag_row, -1)
        lag = lax.broadcasted_iota(jnp.int32, (lags, LANES), 0)
        return jnp.where(lag == wanted, 1.0, 0.0).astype(jnp.bfloat16)

    pick_x = picker(0, 2 * width_x + LANES)
    pick_y = picker(1, width_y + LANES)

    def pick(sums, chosen):
        high = sums.astype(jnp.bfloat16).astype(jnp.float32)
        middle = (sums - high).astype(jnp.bfloat16).astype(jnp.float32)
        low = (sums - high) - middle
        parts = jnp.concatenate([high, middle, low], axis=0).astype(jnp.bfloat16)
        return jnp.dot(parts, chosen, preferred_element_type=jnp.float32)

    load_w.wait()
    lags_z = half + 1
    tile_rows = 8

    def z_step(index, carry):
        start = pl.multiple_of(index * tile_rows, tile_rows)
        rows = [w_own[plane, pl.ds(start, tile_rows), :] for plane in range(planes)]
        return tuple(
            carry[lag] + sum(rows[plane] * rows[plane + lag] for plane in range(planes - lag))
            for lag in range(lags_z)
        )

    zero = jnp.zeros((tile_rows, width_y), jnp.float32)
    z_sums = lax.fori_loop(0, width_x // tile_rows, z_step, (zero,) * lags_z)
    row_z = jnp.zeros((1, LANES), jnp.float32)
    for lag in range(lags_z):
        row_z = jnp.where(lag_row == lag, jnp.sum(z_sums[lag]), row_z)
    row_z = jnp.where((lane >= 2 * FIELD_LANES) & (lane < 3 * FIELD_LANES), row_z, 0.0)

    for copy in places:
        copy.wait()
    for copy in v_copies:
        copy.wait_recv()
    cells = half * width_x
    wide = v_wide[...].reshape(3 * cells, width_y)
    high, low = split(wide)
    left = (high[: 2 * cells], low[: 2 * cells])
    gram_0 = product(left, left, ((0,), (0,)))
    gram_1 = product(left, (high[cells:], low[cells:]), ((0,), (0,)))
    gram_y = jnp.concatenate([gram_0, gram_1], axis=1)
    part = pick(diagonal_sums(gram_y, width_y), pick_y)

    for copy in d_copies:
        copy.wait_recv()
    gram_x = None
    for item in range(quarter):
        for side in range(2):
            for sender in range(2):
                slot = (2 if side == 0 else 0) + sender
                pltpu.make_async_remote_copy(
                    src_ref=u_own.at[0],
                    dst_ref=u_wide.at[side, item, slot],
                    send_sem=u_send.at[side, item, sender],
                    recv_sem=u_recv.at[side, item, sender],
                    device_id={"gx": chip_first + 1 - core},
                    device_id_type=MESH,
                ).wait_recv()
            pair = split(u_wide[side, item].reshape(4 * width_x, width_y))
            lower = (pair[0][: 2 * width_x], pair[1][: 2 * width_x])
            term = product(lower, pair, ((1,), (1,)))
            gram_x = term if gram_x is None else gram_x + term
    part = part + pick(diagonal_sums(gram_x, 2 * width_x), pick_x)
    mine = jnp.sum(part, axis=0, keepdims=True) + row_z

    count = n_gx * n_gy
    me = gx * n_gy + gy
    rows[me] = mine

    def to_device(step):
        peer = lax.rem(me + step, count)
        return pltpu.make_async_remote_copy(
            src_ref=rows.at[me],
            dst_ref=rows.at[me],
            send_sem=row_sem.at[0],
            recv_sem=row_sem.at[1],
            device_id={"gx": peer // n_gy, "gy": lax.rem(peer, n_gy)},
            device_id_type=MESH,
        )

    if count <= 64:
        for step in range(1, count):
            to_device(step).start()
    else:
        lax.fori_loop(1, count, lambda step, _: to_device(step).start(), None)
    all_rows = pltpu.make_async_remote_copy(
        src_ref=rows.at[pl.ds(0, count - 1)],
        dst_ref=rows.at[pl.ds(0, count - 1)],
        send_sem=row_sem.at[0],
        recv_sem=row_sem.at[1],
        device_id={"gx": chip_first + 1 - core},
        device_id_type=MESH,
    )
    all_rows.wait_recv()
    total = jnp.sum(rows[...], axis=0)

    for field in range(3):
        base = FIELD_LANES * field
        row = total[:, base : base + seps] / total[:, base + seps : base + seps + 1]
        if field == 2:
            lag = lag_row[:, base : base + seps].astype(jnp.float32)
            row = row * (jnp.float32(planes) / (jnp.float32(planes) - lag))
        out_ref[field : field + 1, :] = row

    all_rows.wait_send()
    for copy in list(u_copies.values()) + v_copies + d_copies:
        copy.wait_send()


def local(n_gx, n_gy, u_field, v_field, w_field, sep_x, sep_y, sep_z):
    planes, width_x, width_y = u_field.shape
    quarter, half = planes // 4, planes // 2
    seps = sep_x.shape[0]
    dma = pltpu.SemaphoreType.DMA
    block = (planes, width_x, width_y)
    return pl.pallas_call(
        functools.partial(kernel, n_gx, n_gy),
        out_shape=jax.ShapeDtypeStruct((3, seps), jnp.float32),
        in_specs=[pl.BlockSpec(memory_space=pl.ANY)] * 6,
        out_specs=pl.BlockSpec(memory_space=pltpu.VMEM),
        scratch_shapes=[
            pltpu.VMEM(block, jnp.float32),
            pltpu.VMEM(block, jnp.float32),
            pltpu.VMEM(block, jnp.float32),
            pltpu.VMEM((2, quarter, 4, width_x, width_y), jnp.float32),
            pltpu.VMEM((3, half, width_x, width_y), jnp.float32),
            pltpu.SMEM((3, seps), jnp.int32),
            pltpu.VMEM((n_gx * n_gy, 1, LANES), jnp.float32),
            dma((3,)),
            dma((3,)),
            dma((3,)),
            dma((2, quarter, 2)),
            dma((2, quarter, 2)),
            dma((2,)),
            dma((2,)),
            dma((2, half)),
            dma((2, half)),
            dma((2,)),
            pltpu.SemaphoreType.REGULAR((2,)),
            pltpu.SemaphoreType.REGULAR((n_gy // 2,)),
        ],
        compiler_params=pltpu.CompilerParams(collective_id=0, has_side_effects=True),
    )(u_field, v_field, w_field, sep_x, sep_y, sep_z)


def solution(mesh):
    return jax.shard_map(
        functools.partial(local, mesh.shape["gx"], mesh.shape["gy"]),
        mesh=mesh,
        in_specs=(P(None, "gx", "gy"), P(None, "gx", "gy"), P(None, "gx", "gy"), P(), P(), P()),
        out_specs=P(),
        check_vma=False,
    )
```

```python
import functools

import jax
import jax.numpy as jnp
from jax import lax
from jax.experimental import pallas as pl
from jax.experimental.pallas import tpu as pltpu
from jax.sharding import PartitionSpec as P

MESH = pl.DeviceIdType.MESH
LANES = 128
FIELD_LANES = 32


def split(value):
    high = value.astype(jnp.bfloat16)
    low = (value - high.astype(jnp.float32)).astype(jnp.bfloat16)
    return high, low


def product(left, right, dims):
    dot = functools.partial(
        lax.dot_general, dimension_numbers=(dims, ((), ())), preferred_element_type=jnp.float32
    )
    return dot(left[0], right[0]) + (dot(left[0], right[1]) + dot(left[1], right[0]))


def diagonal_sums(gram, largest):
    rows = gram.shape[0]
    window = largest + LANES
    folded = gram[:LANES, :window]
    for start in range(LANES, rows, LANES):
        folded = folded + gram[start : start + LANES, start : start + window]
    total = folded[:8]
    for start in range(8, LANES, 8):
        total = total + pltpu.roll(folded[start : start + 8], window - start, 1)
    row = lax.broadcasted_iota(jnp.int32, total.shape, 0)
    for bit in (1, 2, 4):
        total = jnp.where((row & bit) != 0, pltpu.roll(total, window - bit, 1), total)
    return total


def kernel(
    n_gx, n_gy,
    u_hbm, v_hbm, w_hbm, sep_x_hbm, sep_y_hbm, sep_z_hbm, out_ref,
    u_own, v_own, w_own, u_wide, v_wide, sep_s, rows,
    plane_sem, load_sem, sep_sem, place_sem, u_send, u_recv, d_send, d_recv, v_send, v_recv,
    row_sem, line_sem, pair_sem,
):
    planes, width_x, width_y = u_own.shape
    seps = sep_s.shape[1]
    quarter, half = planes // 4, planes // 2
    gx, gy = lax.axis_index("gx"), lax.axis_index("gy")
    core, parity = lax.rem(gx, 2), lax.rem(gy, 2)
    chip_first = gx - core

    order = [quarter * part + item for item in range(quarter) for part in range(4)]
    load_u = {
        plane: pltpu.make_async_copy(u_hbm.at[plane], u_own.at[plane], plane_sem.at[plane])
        for plane in order
    }
    load_v = pltpu.make_async_copy(v_hbm, v_own, load_sem.at[0])
    load_w = pltpu.make_async_copy(w_hbm, w_own, load_sem.at[1])
    for plane in order:
        load_u[plane].start()
    load_v.start()

    chip, chips = gx // 2, n_gx // 2
    first, last = chip == 0, chip == chips - 1
    near = gy + 1 - 2 * parity
    far_to = lax.rem(gy + n_gy - 2 + 4 * parity, n_gy)
    far_from = lax.rem(gy + n_gy + 2 - 4 * parity, n_gy)
    barrier = pltpu.get_barrier_semaphore()

    def greet(semaphore, **device):
        pl.semaphore_signal(semaphore, inc=1, device_id=device, device_id_type=MESH)

    @pl.when(~first)
    def _():
        greet(barrier, gx=chip_first - 2)
        greet(barrier, gx=chip_first - 1)

    @pl.when(~last)
    def _():
        greet(barrier, gx=chip_first + 2)
        greet(barrier, gx=chip_first + 3)

    greet(barrier, gx=chip_first + 1 - core)
    greet(barrier, gy=near)
    greet(barrier, gy=far_from)
    load_w.start()
    sep_loads = [
        pltpu.make_async_copy(ref, sep_s.at[index], sep_sem.at[index])
        for index, ref in enumerate((sep_x_hbm, sep_y_hbm, sep_z_hbm))
    ]
    places = []
    for side in range(2):
        places.append(pltpu.make_async_copy(
            u_hbm.at[pl.ds(half * side + quarter * core, quarter)],
            u_wide.at[side, :, 2 * side + core],
            place_sem.at[side],
        ))
    places.append(pltpu.make_async_copy(
        v_hbm.at[pl.ds(half * parity, half)], v_wide.at[2 * parity], place_sem.at[2]
    ))
    for copy in places + sep_loads:
        copy.start()

    u_copies = {}
    for item in range(quarter):
        for other in range(2):
            for side in range(2):
                target = lax.rem(chip_first + (n_gx - 2 if side == 0 else 2), n_gx)
                u_copies[side, item, other] = (pltpu.make_async_remote_copy(
                    src_ref=u_own.at[half * side + quarter * other + item],
                    dst_ref=u_wide.at[side, item, (2 if side == 0 else 0) + core],
                    send_sem=u_send.at[side, item, other],
                    recv_sem=u_recv.at[side, item, core],
                    device_id={"gx": target + other},
                    device_id_type=MESH,
                ))
    d_copies = []
    for side in range(2):
        d_copies.append(pltpu.make_async_remote_copy(
            src_ref=u_own.at[pl.ds(half * side + quarter * (1 - core), quarter)],
            dst_ref=u_wide.at[side, :, 2 * side + core],
            send_sem=d_send.at[side],
            recv_sem=d_recv.at[side],
            device_id={"gx": chip_first + 1 - core},
            device_id_type=MESH,
        ))
    v_copies = []
    for item in range(half):
        v_copies.append(pltpu.make_async_remote_copy(
            src_ref=v_own.at[half * (1 - parity) + item],
            dst_ref=v_wide.at[1, item],
            send_sem=v_send.at[0, item],
            recv_sem=v_recv.at[0, item],
            device_id={"gy": near},
            device_id_type=MESH,
        ))
        v_copies.append(pltpu.make_async_remote_copy(
            src_ref=v_own.at[half * parity + item],
            dst_ref=v_wide.at[2 - 2 * parity, item],
            send_sem=v_send.at[1, item],
            recv_sem=v_recv.at[1, item],
            device_id={"gy": far_to},
            device_id_type=MESH,
        ))

    for plane in order[:4]:
        load_u[plane].wait()
    inner = jnp.where(first, 0, 2) + jnp.where(last, 0, 2)
    pl.semaphore_wait(barrier, inner + 3)

    def start_u(side, items, at_end):
        wraps = first if side == 0 else last

        @pl.when(wraps if at_end else ~wraps)
        def _():
            for item in items:
                for other in range(2):
                    u_copies[side, item, other].start()

    for side in range(2):
        start_u(side, range(1), False)
    for plane in order[4:]:
        load_u[plane].wait()
    load_v.wait()
    for copy in v_copies + d_copies:
        copy.start()

    up, down = line_sem.at[0], line_sem.at[1]

    @pl.when(chip == 1)
    def _():
        greet(up, gx=gx + 2)

    @pl.when(chip == chips - 2)
    def _():
        greet(down, gx=gx - 2)

    @pl.when(chip >= 2)
    def _():
        pl.semaphore_wait(up, 1)

    @pl.when((chip >= 2) & (chip <= chips - 2))
    def _():
        greet(up, gx=gx + 2)

    @pl.when(chip <= chips - 3)
    def _():
        pl.semaphore_wait(down, 1)

    @pl.when((chip >= 1) & (chip <= chips - 3))
    def _():
        greet(down, gx=gx - 2)

    for side in range(2):
        start_u(side, range(quarter), True)
    for side in range(2):
        start_u(side, range(1, quarter), False)

    greet(pair_sem.at[0], gy=near)
    pl.semaphore_wait(pair_sem.at[0], 1)
    for hop in range(1, n_gy // 2):
        greet(pair_sem.at[hop], gy=far_from)
        pl.semaphore_wait(pair_sem.at[hop], 1)

    for copy in sep_loads:
        copy.wait()
    lane = lax.broadcasted_iota(jnp.int32, (1, LANES), 1)
    lag_row = jnp.full((1, LANES), -1, jnp.int32)
    for field in range(3):
        for index in range(seps):
            lag_row = jnp.where(lane == FIELD_LANES * field + index, sep_s[field, index], lag_row)
        lag_row = jnp.where(lane == FIELD_LANES * field + seps, 0, lag_row)

    def picker(field, lags):
        of_field = (lane >= FIELD_LANES * field) & (lane < FIELD_LANES * (field + 1))
        wanted = jnp.where(of_field, lag_row, -1)
        lag = lax.broadcasted_iota(jnp.int32, (lags, LANES), 0)
        return jnp.where(lag == wanted, 1.0, 0.0).astype(jnp.bfloat16)

    pick_x = picker(0, 2 * width_x + LANES)
    pick_y = picker(1, width_y + LANES)

    def pick(sums, chosen):
        high = sums.astype(jnp.bfloat16).astype(jnp.float32)
        middle = (sums - high).astype(jnp.bfloat16).astype(jnp.float32)
        low = (sums - high) - middle
        parts = jnp.concatenate([high, middle, low], axis=0).astype(jnp.bfloat16)
        return jnp.dot(parts, chosen, preferred_element_type=jnp.float32)

    load_w.wait()
    lags_z = half + 1
    tile_rows = 8

    def z_step(index, carry):
        start = pl.multiple_of(index * tile_rows, tile_rows)
        rows = [w_own[plane, pl.ds(start, tile_rows), :] for plane in range(planes)]
        return tuple(
            carry[lag] + sum(rows[plane] * rows[plane + lag] for plane in range(planes - lag))
            for lag in range(lags_z)
        )

    zero = jnp.zeros((tile_rows, width_y), jnp.float32)
    z_sums = lax.fori_loop(0, width_x // tile_rows, z_step, (zero,) * lags_z)
    row_z = jnp.zeros((1, LANES), jnp.float32)
    for lag in range(lags_z):
        row_z = jnp.where(lag_row == lag, jnp.sum(z_sums[lag]), row_z)
    row_z = jnp.where((lane >= 2 * FIELD_LANES) & (lane < 3 * FIELD_LANES), row_z, 0.0)

    for copy in places:
        copy.wait()
    for copy in v_copies:
        copy.wait_recv()
    cells = half * width_x
    wide = v_wide[...].reshape(3 * cells, width_y)
    high, low = split(wide)
    left = (high[: 2 * cells], low[: 2 * cells])
    gram_0 = product(left, left, ((0,), (0,)))
    gram_1 = product(left, (high[cells:], low[cells:]), ((0,), (0,)))
    gram_y = jnp.concatenate([gram_0, gram_1], axis=1)
    part = pick(diagonal_sums(gram_y, width_y), pick_y)

    for copy in d_copies:
        copy.wait_recv()
    gram_x = None
    for item in range(quarter):
        for side in range(2):
            for sender in range(2):
                slot = (2 if side == 0 else 0) + sender
                pltpu.make_async_remote_copy(
                    src_ref=u_own.at[0],
                    dst_ref=u_wide.at[side, item, slot],
                    send_sem=u_send.at[side, item, sender],
                    recv_sem=u_recv.at[side, item, sender],
                    device_id={"gx": chip_first + 1 - core},
                    device_id_type=MESH,
                ).wait_recv()
            pair = split(u_wide[side, item].reshape(4 * width_x, width_y))
            lower = (pair[0][: 2 * width_x], pair[1][: 2 * width_x])
            term = product(lower, pair, ((1,), (1,)))
            gram_x = term if gram_x is None else gram_x + term
    part = part + pick(diagonal_sums(gram_x, 2 * width_x), pick_x)
    mine = jnp.sum(part, axis=0, keepdims=True) + row_z

    count = n_gx * n_gy
    me = gx * n_gy + gy
    rows[me] = mine

    flips = [(1 - 2 * lax.rem(me // (1 << bit), 2)) * (1 << bit) for bit in range(count.bit_length() - 1)]
    by_flips = count == 1 << len(flips)

    def to_device(step):
        if by_flips and isinstance(step, int):
            peer = me + sum(flip for bit, flip in enumerate(flips) if step >> bit & 1)
        else:
            peer = lax.rem(me + step, count)
        return pltpu.make_async_remote_copy(
            src_ref=rows.at[me],
            dst_ref=rows.at[me],
            send_sem=row_sem.at[0],
            recv_sem=row_sem.at[1],
            device_id={"gx": peer // n_gy, "gy": lax.rem(peer, n_gy)},
            device_id_type=MESH,
        )

    if count <= 64:
        for step in reversed(range(1, count)):
            to_device(step).start()
    else:
        lax.fori_loop(1, count, lambda step, _: to_device(step).start(), None)
    all_rows = pltpu.make_async_remote_copy(
        src_ref=rows.at[pl.ds(0, count - 1)],
        dst_ref=rows.at[pl.ds(0, count - 1)],
        send_sem=row_sem.at[0],
        recv_sem=row_sem.at[1],
        device_id={"gx": chip_first + 1 - core},
        device_id_type=MESH,
    )
    all_rows.wait_recv()
    total = jnp.sum(rows[...], axis=0)

    for field in range(3):
        base = FIELD_LANES * field
        row = total[:, base : base + seps] / total[:, base + seps : base + seps + 1]
        if field == 2:
            lag = lag_row[:, base : base + seps].astype(jnp.float32)
            row = row * (jnp.float32(planes) / (jnp.float32(planes) - lag))
        out_ref[field : field + 1, :] = row

    all_rows.wait_send()
    for copy in list(u_copies.values()) + v_copies + d_copies:
        copy.wait_send()


def local(n_gx, n_gy, u_field, v_field, w_field, sep_x, sep_y, sep_z):
    planes, width_x, width_y = u_field.shape
    quarter, half = planes // 4, planes // 2
    seps = sep_x.shape[0]
    dma = pltpu.SemaphoreType.DMA
    block = (planes, width_x, width_y)
    return pl.pallas_call(
        functools.partial(kernel, n_gx, n_gy),
        out_shape=pltpu.VMEM((3, seps), jnp.float32),
        in_specs=[pl.BlockSpec(memory_space=pl.ANY)] * 6,
        out_specs=pl.BlockSpec(memory_space=pltpu.VMEM),
        scratch_shapes=[
            pltpu.VMEM(block, jnp.float32),
            pltpu.VMEM(block, jnp.float32),
            pltpu.VMEM(block, jnp.float32),
            pltpu.VMEM((2, quarter, 4, width_x, width_y), jnp.float32),
            pltpu.VMEM((3, half, width_x, width_y), jnp.float32),
            pltpu.SMEM((3, seps), jnp.int32),
            pltpu.VMEM((n_gx * n_gy, 1, LANES), jnp.float32),
            dma((planes,)),
            dma((2,)),
            dma((3,)),
            dma((3,)),
            dma((2, quarter, 2)),
            dma((2, quarter, 2)),
            dma((2,)),
            dma((2,)),
            dma((2, half)),
            dma((2, half)),
            dma((2,)),
            pltpu.SemaphoreType.REGULAR((2,)),
            pltpu.SemaphoreType.REGULAR((n_gy // 2,)),
        ],
        compiler_params=pltpu.CompilerParams(collective_id=0, has_side_effects=True),
    )(u_field, v_field, w_field, sep_x, sep_y, sep_z)


def solution(mesh):
    return jax.shard_map(
        functools.partial(local, mesh.shape["gx"], mesh.shape["gy"]),
        mesh=mesh,
        in_specs=(P(None, "gx", "gy"), P(None, "gx", "gy"), P(None, "gx", "gy"), P(), P(), P()),
        out_specs=P(),
        check_vma=False,
    )
```

```python
import functools

import jax
import jax.numpy as jnp
from jax import lax
from jax.experimental import pallas as pl
from jax.experimental.pallas import tpu as pltpu
from jax.sharding import PartitionSpec as P

MESH = pl.DeviceIdType.MESH
LANES = 128
FIELD_LANES = 32


def split(value):
    high = value.astype(jnp.bfloat16)
    low = (value - high.astype(jnp.float32)).astype(jnp.bfloat16)
    return high, low


def product(left, right, dims):
    dot = functools.partial(
        lax.dot_general, dimension_numbers=(dims, ((), ())), preferred_element_type=jnp.float32
    )
    return dot(left[0], right[0]) + (dot(left[0], right[1]) + dot(left[1], right[0]))


def diagonal_sums(gram, largest):
    rows = gram.shape[0]
    window = largest + LANES
    folded = gram[:LANES, :window]
    for start in range(LANES, rows, LANES):
        folded = folded + gram[start : start + LANES, start : start + window]
    total = folded[:8]
    for start in range(8, LANES, 8):
        total = total + pltpu.roll(folded[start : start + 8], window - start, 1)
    row = lax.broadcasted_iota(jnp.int32, total.shape, 0)
    for bit in (1, 2, 4):
        total = jnp.where((row & bit) != 0, pltpu.roll(total, window - bit, 1), total)
    return total


def kernel(
    n_gx, n_gy,
    u_hbm, v_hbm, w_hbm, sep_x_hbm, sep_y_hbm, sep_z_hbm, out_ref,
    u_own, v_own, w_own, u_wide, v_wide, sep_s, rows,
    plane_sem, load_sem, sep_sem, place_sem, u_send, u_recv, d_send, d_recv, v_send, v_recv,
    row_sem, line_sem, pair_sem,
):
    planes, width_x, width_y = u_own.shape
    seps = sep_s.shape[1]
    quarter, half = planes // 4, planes // 2
    gx, gy = lax.axis_index("gx"), lax.axis_index("gy")
    core, parity = lax.rem(gx, 2), lax.rem(gy, 2)
    chip_first = gx - core

    order = [quarter * part + item for item in range(quarter) for part in range(4)]
    load_u = {
        plane: pltpu.make_async_copy(u_hbm.at[plane], u_own.at[plane], plane_sem.at[plane])
        for plane in order
    }
    load_v = pltpu.make_async_copy(v_hbm, v_own, load_sem.at[0])
    load_w = pltpu.make_async_copy(w_hbm, w_own, load_sem.at[1])
    for plane in order:
        load_u[plane].start()
    load_v.start()

    chip, chips = gx // 2, n_gx // 2
    first, last = chip == 0, chip == chips - 1
    near = gy + 1 - 2 * parity
    far_to = lax.rem(gy + n_gy - 2 + 4 * parity, n_gy)
    far_from = lax.rem(gy + n_gy + 2 - 4 * parity, n_gy)
    barrier = pltpu.get_barrier_semaphore()

    def greet(semaphore, **device):
        pl.semaphore_signal(semaphore, inc=1, device_id=device, device_id_type=MESH)

    @pl.when(~first)
    def _():
        greet(barrier, gx=chip_first - 2)
        greet(barrier, gx=chip_first - 1)

    @pl.when(~last)
    def _():
        greet(barrier, gx=chip_first + 2)
        greet(barrier, gx=chip_first + 3)

    greet(barrier, gx=chip_first + 1 - core)
    greet(barrier, gy=near)
    greet(barrier, gy=far_from)
    load_w.start()
    sep_loads = [
        pltpu.make_async_copy(ref, sep_s.at[index], sep_sem.at[index])
        for index, ref in enumerate((sep_x_hbm, sep_y_hbm, sep_z_hbm))
    ]
    places = []
    for side in range(2):
        places.append(pltpu.make_async_copy(
            u_hbm.at[pl.ds(half * side + quarter * core, quarter)],
            u_wide.at[side, :, 2 * side + core],
            place_sem.at[side],
        ))
    places.append(pltpu.make_async_copy(
        v_hbm.at[pl.ds(half * parity, half)], v_wide.at[2 * parity], place_sem.at[2]
    ))
    for copy in places + sep_loads:
        copy.start()

    u_copies = {}
    for item in range(quarter):
        for other in range(2):
            for side in range(2):
                target = lax.rem(chip_first + (n_gx - 2 if side == 0 else 2), n_gx)
                u_copies[side, item, other] = (pltpu.make_async_remote_copy(
                    src_ref=u_own.at[half * side + quarter * other + item],
                    dst_ref=u_wide.at[side, item, (2 if side == 0 else 0) + core],
                    send_sem=u_send.at[side, item, other],
                    recv_sem=u_recv.at[side, item, core],
                    device_id={"gx": target + other},
                    device_id_type=MESH,
                ))
    d_copies = []
    for side in range(2):
        d_copies.append(pltpu.make_async_remote_copy(
            src_ref=u_own.at[pl.ds(half * side + quarter * (1 - core), quarter)],
            dst_ref=u_wide.at[side, :, 2 * side + core],
            send_sem=d_send.at[side],
            recv_sem=d_recv.at[side],
            device_id={"gx": chip_first + 1 - core},
            device_id_type=MESH,
        ))
    v_copies = []
    for item in range(half):
        v_copies.append(pltpu.make_async_remote_copy(
            src_ref=v_own.at[half * (1 - parity) + item],
            dst_ref=v_wide.at[1, item],
            send_sem=v_send.at[0, item],
            recv_sem=v_recv.at[0, item],
            device_id={"gy": near},
            device_id_type=MESH,
        ))
        v_copies.append(pltpu.make_async_remote_copy(
            src_ref=v_own.at[half * parity + item],
            dst_ref=v_wide.at[2 - 2 * parity, item],
            send_sem=v_send.at[1, item],
            recv_sem=v_recv.at[1, item],
            device_id={"gy": far_to},
            device_id_type=MESH,
        ))

    for plane in order[:4]:
        load_u[plane].wait()
    inner = jnp.where(first, 0, 2) + jnp.where(last, 0, 2)
    pl.semaphore_wait(barrier, inner + 3)

    def start_u(side, items, at_end):
        wraps = first if side == 0 else last

        @pl.when(wraps if at_end else ~wraps)
        def _():
            for item in items:
                for other in range(2):
                    u_copies[side, item, other].start()

    ends = first | last
    for side in range(2):
        start_u(side, range(1), False)
    for plane in order[4:]:
        load_u[plane].wait()
    @pl.when(~ends)
    def _():
        for side in range(2):
            for item in range(1, quarter):
                for other in range(2):
                    u_copies[side, item, other].start()
    load_v.wait()
    for copy in v_copies + d_copies:
        copy.start()

    up, down = line_sem.at[0], line_sem.at[1]

    @pl.when(chip == 1)
    def _():
        greet(up, gx=gx + 2)

    @pl.when(chip == chips - 2)
    def _():
        greet(down, gx=gx - 2)

    @pl.when(chip >= 2)
    def _():
        pl.semaphore_wait(up, 1)

    @pl.when((chip >= 2) & (chip <= chips - 2))
    def _():
        greet(up, gx=gx + 2)

    @pl.when(chip <= chips - 3)
    def _():
        pl.semaphore_wait(down, 1)

    @pl.when((chip >= 1) & (chip <= chips - 3))
    def _():
        greet(down, gx=gx - 2)

    for side in range(2):
        start_u(side, range(quarter), True)
    @pl.when(ends)
    def _():
        for side in range(2):
            start_u(side, range(1, quarter), False)

    greet(pair_sem.at[0], gy=near)
    pl.semaphore_wait(pair_sem.at[0], 1)
    for hop in range(1, n_gy // 2):
        greet(pair_sem.at[hop], gy=far_from)
        pl.semaphore_wait(pair_sem.at[hop], 1)

    for copy in sep_loads:
        copy.wait()
    lane = lax.broadcasted_iota(jnp.int32, (1, LANES), 1)
    lag_row = jnp.full((1, LANES), -1, jnp.int32)
    for field in range(3):
        for index in range(seps):
            lag_row = jnp.where(lane == FIELD_LANES * field + index, sep_s[field, index], lag_row)
        lag_row = jnp.where(lane == FIELD_LANES * field + seps, 0, lag_row)

    def picker(field, lags):
        of_field = (lane >= FIELD_LANES * field) & (lane < FIELD_LANES * (field + 1))
        wanted = jnp.where(of_field, lag_row, -1)
        lag = lax.broadcasted_iota(jnp.int32, (lags, LANES), 0)
        return jnp.where(lag == wanted, 1.0, 0.0).astype(jnp.bfloat16)

    pick_x = picker(0, 2 * width_x + LANES)
    pick_y = picker(1, width_y + LANES)

    def pick(sums, chosen):
        high = sums.astype(jnp.bfloat16).astype(jnp.float32)
        middle = (sums - high).astype(jnp.bfloat16).astype(jnp.float32)
        low = (sums - high) - middle
        parts = jnp.concatenate([high, middle, low], axis=0).astype(jnp.bfloat16)
        return jnp.dot(parts, chosen, preferred_element_type=jnp.float32)

    load_w.wait()
    lags_z = half + 1
    tile_rows = 8

    def z_step(index, carry):
        start = pl.multiple_of(index * tile_rows, tile_rows)
        rows = [w_own[plane, pl.ds(start, tile_rows), :] for plane in range(planes)]
        return tuple(
            carry[lag] + sum(rows[plane] * rows[plane + lag] for plane in range(planes - lag))
            for lag in range(lags_z)
        )

    zero = jnp.zeros((tile_rows, width_y), jnp.float32)
    z_sums = lax.fori_loop(0, width_x // tile_rows, z_step, (zero,) * lags_z)
    row_z = jnp.zeros((1, LANES), jnp.float32)
    for lag in range(lags_z):
        row_z = jnp.where(lag_row == lag, jnp.sum(z_sums[lag]), row_z)
    row_z = jnp.where((lane >= 2 * FIELD_LANES) & (lane < 3 * FIELD_LANES), row_z, 0.0)

    for copy in places:
        copy.wait()
    for copy in v_copies:
        copy.wait_recv()
    cells = half * width_x
    wide = v_wide[...].reshape(3 * cells, width_y)
    high, low = split(wide)
    left = (high[: 2 * cells], low[: 2 * cells])
    gram_0 = product(left, left, ((0,), (0,)))
    gram_1 = product(left, (high[cells:], low[cells:]), ((0,), (0,)))
    gram_y = jnp.concatenate([gram_0, gram_1], axis=1)
    rest = jnp.sum(pick(diagonal_sums(gram_y, width_y), pick_y), axis=0, keepdims=True) + row_z

    for copy in d_copies:
        copy.wait_recv()
    gram_x = None
    for item in range(quarter):
        for side in range(2):
            for sender in range(2):
                slot = (2 if side == 0 else 0) + sender
                pltpu.make_async_remote_copy(
                    src_ref=u_own.at[0],
                    dst_ref=u_wide.at[side, item, slot],
                    send_sem=u_send.at[side, item, sender],
                    recv_sem=u_recv.at[side, item, sender],
                    device_id={"gx": chip_first + 1 - core},
                    device_id_type=MESH,
                ).wait_recv()
            pair = split(u_wide[side, item].reshape(4 * width_x, width_y))
            lower = (pair[0][: 2 * width_x], pair[1][: 2 * width_x])
            term = product(lower, pair, ((1,), (1,)))
            gram_x = term if gram_x is None else gram_x + term
    mine = jnp.sum(pick(diagonal_sums(gram_x, 2 * width_x), pick_x), axis=0, keepdims=True) + rest

    count = n_gx * n_gy
    me = gx * n_gy + gy
    rows[me] = mine

    flips = [(1 - 2 * lax.rem(me // (1 << bit), 2)) * (1 << bit) for bit in range(count.bit_length() - 1)]
    by_flips = count == 1 << len(flips)

    def to_device(step):
        if by_flips and isinstance(step, int):
            peer = me + sum(flip for bit, flip in enumerate(flips) if step >> bit & 1)
        else:
            peer = lax.rem(me + step, count)
        return pltpu.make_async_remote_copy(
            src_ref=rows.at[me],
            dst_ref=rows.at[me],
            send_sem=row_sem.at[0],
            recv_sem=row_sem.at[1],
            device_id={"gx": peer // n_gy, "gy": lax.rem(peer, n_gy)},
            device_id_type=MESH,
        )

    if count <= 64:
        for step in reversed(range(1, count)):
            to_device(step).start()
    else:
        lax.fori_loop(1, count, lambda step, _: to_device(step).start(), None)
    all_rows = pltpu.make_async_remote_copy(
        src_ref=rows.at[pl.ds(0, count - 1)],
        dst_ref=rows.at[pl.ds(0, count - 1)],
        send_sem=row_sem.at[0],
        recv_sem=row_sem.at[1],
        device_id={"gx": chip_first + 1 - core},
        device_id_type=MESH,
    )
    all_rows.wait_recv()
    total = jnp.sum(rows[...], axis=0)

    for field in range(3):
        base = FIELD_LANES * field
        row = total[:, base : base + seps] / total[:, base + seps : base + seps + 1]
        if field == 2:
            lag = lag_row[:, base : base + seps].astype(jnp.float32)
            row = row * (jnp.float32(planes) / (jnp.float32(planes) - lag))
        out_ref[field : field + 1, :] = row

    all_rows.wait_send()
    for copy in list(u_copies.values()) + v_copies + d_copies:
        copy.wait_send()


def local(n_gx, n_gy, u_field, v_field, w_field, sep_x, sep_y, sep_z):
    planes, width_x, width_y = u_field.shape
    quarter, half = planes // 4, planes // 2
    seps = sep_x.shape[0]
    dma = pltpu.SemaphoreType.DMA
    block = (planes, width_x, width_y)
    return pl.pallas_call(
        functools.partial(kernel, n_gx, n_gy),
        out_shape=pltpu.VMEM((3, seps), jnp.float32),
        in_specs=[pl.BlockSpec(memory_space=pl.ANY)] * 6,
        out_specs=pl.BlockSpec(memory_space=pltpu.VMEM),
        scratch_shapes=[
            pltpu.VMEM(block, jnp.float32),
            pltpu.VMEM(block, jnp.float32),
            pltpu.VMEM(block, jnp.float32),
            pltpu.VMEM((2, quarter, 4, width_x, width_y), jnp.float32),
            pltpu.VMEM((3, half, width_x, width_y), jnp.float32),
            pltpu.SMEM((3, seps), jnp.int32),
            pltpu.VMEM((n_gx * n_gy, 1, LANES), jnp.float32),
            dma((planes,)),
            dma((2,)),
            dma((3,)),
            dma((3,)),
            dma((2, quarter, 2)),
            dma((2, quarter, 2)),
            dma((2,)),
            dma((2,)),
            dma((2, half)),
            dma((2, half)),
            dma((2,)),
            pltpu.SemaphoreType.REGULAR((2,)),
            pltpu.SemaphoreType.REGULAR((n_gy // 2,)),
        ],
        compiler_params=pltpu.CompilerParams(collective_id=0, has_side_effects=True),
    )(u_field, v_field, w_field, sep_x, sep_y, sep_z)


def solution(mesh):
    return jax.shard_map(
        functools.partial(local, mesh.shape["gx"], mesh.shape["gy"]),
        mesh=mesh,
        in_specs=(P(None, "gx", "gy"), P(None, "gx", "gy"), P(None, "gx", "gy"), P(), P(), P()),
        out_specs=P(),
        check_vma=False,
    )
```
